32 devices in a mesh: rep: 1, ep: 32 (over z, y, x, core).
Axes of the slice: x: 2, y: 2, z: 4, core: 2. Of those that a mesh axis runs over, the one named last changes fastest.
Arguments:
- tokens: bfloat16 [512, 3584], P(('rep', 'ep')), may hold values from -6 to 6
- routes: int32 [512, 8], P(('rep', 'ep')), may hold values from 0 to 15, all different within a row; in each aligned block of 16 rows (0 to 15, 16 to 31, ...) at most 16 rows name the same one
- gate_weights: float32 [512, 8], P(('rep', 'ep')), may hold values from 0.05 to 0.5
- w_gate: bfloat16 [32, 3584, 512], P('ep'), may hold values from -0.09375 to 0.09375
- w_up: bfloat16 [32, 3584, 512], P('ep'), may hold values from -0.09375 to 0.09375
- w_down: bfloat16 [32, 512, 3584], P('ep'), may hold values from -0.1875 to 0.1875
Outputs:
- mixed: bfloat16 [512, 3584], P(('rep', 'ep'))
The draws below stay inside these ranges and needn't reach their ends.
Inputs may be any that keep to these rules, and one draw needn't show every extreme that they name: `routes`: each token names 8 different experts. Among the tokens of one device at most 16 name any one expert, and in every draw some expert is named by exactly 16 tokens of some device.
All inputs are finite; a program needn't handle non-finite values.
Results may differ from the reference program's by a relative error of at most 0.008.
Values may be sent and summed in bfloat16 or wider, within the bound.
A program may use at most 128 MiB of HBM per device.

```python
import math
import jax
import jax.numpy as jnp
import numpy as np
from jax import lax

D = 3584
FF = 1024
TOP = 8
TOK_DEV = 16
EXPERTS = 16
CAP = 16
TOKENS = 512
N_EP = 32


def steps_of(stream_key, extent, pieces, smallest, largest):
    gain, own = 1.0, jax.random.fold_in(stream_key, 6)
    for dim, shards_of in pieces:
        draws = jnp.exp(jax.random.uniform(jax.random.fold_in(own, dim), (shards_of,), jnp.float32, smallest / len(pieces), largest / len(pieces)))
        gain = gain * jnp.repeat(draws, extent[dim] // shards_of).reshape([-1 if axis == dim else 1 for axis in range(len(extent))])
    return gain


def assign_block(stream_key, own, number, rows, count, top, limit, lean):
    order = jax.random.permutation(stream_key, count)
    packed, usual = shares(count, rows * top, limit, lean, True), shares(count, rows * top, limit, lean, False)
    places = jnp.arange(count)

    def named(tallies, rotation):
        used = int((tallies > 0).sum())
        fixed = max(1, used // 4)
        moved = fixed + (places - fixed + rotation * (used - fixed)) % max(1, count - fixed)
        return jnp.zeros((count,), jnp.int32).at[order[jnp.where(places < fixed, places, moved)]].set(jnp.asarray(tallies, jnp.int32))

    tallies = jnp.where(number % 4 == 0, named(packed, number // 4), named(usual, number - number // 4 - 1))
    mixed = jax.random.permutation(jax.random.fold_in(own, 3), count)
    giver, sink = mixed[0:count // 2 * 2:2], mixed[1:count // 2 * 2:2]
    margin = jnp.minimum(tallies[giver] - 1, limit - tallies[sink]) // 2
    margin = jnp.where((giver == order[0]) | (sink == order[0]) | (tallies[sink] == 0), 0, jnp.maximum(margin, 0))
    moved = jax.random.randint(jax.random.fold_in(own, 4), (count // 2,), 0, 1 << 20) % (margin + 1)
    tallies = tallies.at[giver].add(-moved).at[sink].add(moved)
    items = jnp.searchsorted(jnp.cumsum(tallies), jnp.arange(rows * top), side="right").astype(jnp.int32)
    listing = items.reshape(top, rows).T
    listing = listing[jax.random.permutation(jax.random.fold_in(own, 1), rows)]
    rotation = jax.random.randint(jax.random.fold_in(own, 2), (rows, 1), 0, top)
    return jnp.take_along_axis(listing, (jnp.arange(top)[None, :] + rotation) % top, axis=1)


def shares(number_of, total, limit, skew, full):
    weights = [(1 << 20) // math.isqrt(standing ** skew) + 1 for standing in range(1, number_of + 1)]
    largest = limit if full else min(limit, max(-(-total // number_of), total * weights[0] // sum(weights)))
    least = 1 if total - largest >= number_of - 1 else 0
    holding, surplus = [largest] + [least] * (number_of - 1), total - largest - least * (number_of - 1)
    while surplus > 0:
        free = [i for i in range(1, number_of) if holding[i] < largest] or [i for i in range(1, number_of) if holding[i] < limit]
        whole, remaining = sum([weights[i] for i in free]), surplus
        for i in free:
            more = min(limit - holding[i], max(1, remaining * weights[i] // whole), surplus)
            holding[i] = holding[i] + more
            surplus = surplus - more
    return np.array(holding)


def gaussian(rng, extent, scale, bound, cuts=(), kind=jnp.bfloat16):
    gain = steps_of(rng, extent, cuts, -0.22, 0.18) if cuts else 1.0
    values = jax.random.normal(rng, extent, jnp.float32) * scale * gain
    return jnp.minimum(jnp.maximum(values, -bound), bound).astype(kind)


def setup_inputs(seed: int = 0, part: int = 0) -> dict:
    keys = jax.random.split(jax.random.key(seed), 7)
    own_keys = jax.random.split(jax.random.fold_in(keys[6], part), 7)
    tokens = gaussian(own_keys[0], (TOKENS, D), 1.0, 6.0, ((0, 32),))
    routes_keys = jax.random.split(jax.random.fold_in(own_keys[1], 1), TOKENS // TOK_DEV)
    routes_turns = jax.random.permutation(jax.random.fold_in(own_keys[1], 3), TOKENS // TOK_DEV)
    routes = jax.vmap(lambda own, number: assign_block(jax.random.fold_in(own_keys[1], 2), own, number, TOK_DEV, EXPERTS, TOP, CAP, 2))(routes_keys, routes_turns).reshape((TOKENS, TOP))
    gate_weights = jnp.clip(0.05 + 0.45 * jax.random.uniform(own_keys[2], (TOKENS, TOP), jnp.float32) ** steps_of(own_keys[2], (TOKENS, TOP), ((0, 32),), -0.2, 0.2), 0.05, 0.5)
    w_gate = gaussian(keys[3], (2 * EXPERTS, D, FF // 2), D ** -0.5, 0.09375, ((0, 32),))
    w_up = gaussian(keys[4], (2 * EXPERTS, D, FF // 2), D ** -0.5, 0.09375, ((0, 32),))
    w_down = gaussian(keys[5], (2 * EXPERTS, FF // 2, D), FF ** -0.5, 0.1875, ((0, 32),))
    return {"tokens": tokens, "routes": routes, "gate_weights": gate_weights, "w_gate": w_gate, "w_up": w_up, "w_down": w_down}


def slot_positions(chosen, expert_count):
    chosen_hits = jnp.sum((chosen[:, :, None] == jnp.arange(expert_count, dtype=jnp.int32)[None, None, :]).astype(jnp.int32), axis=1, dtype=jnp.int32)
    before = (jnp.cumsum(chosen_hits, axis=0, dtype=jnp.int32) - chosen_hits).astype(jnp.int32)
    return jnp.take_along_axis(before, chosen, axis=1).astype(jnp.int32)


def reference(tokens, routes, gate_weights, w_gate, w_up, w_down):
    block_tokens = tokens.reshape(N_EP, TOK_DEV, D)
    block_routes = routes.reshape(N_EP, TOK_DEV, TOP).astype(jnp.int32)

    def fill_block(token_rows, chosen):
        slot_index = slot_positions(chosen, EXPERTS)
        flat_index = (chosen * CAP + slot_index).reshape(-1).astype(jnp.int32)
        buffer = jnp.zeros((EXPERTS * CAP, D), tokens.dtype).at[flat_index].set(jnp.repeat(token_rows, TOP, axis=0))
        return buffer.reshape(EXPERTS, CAP, D), flat_index

    buffers, flat_all = jax.vmap(fill_block)(block_tokens, block_routes)
    gate_halves = w_gate.reshape(EXPERTS, 2, D, FF // 2)
    up_halves = w_up.reshape(EXPERTS, 2, D, FF // 2)
    down_halves = w_down.reshape(EXPERTS, 2, FF // 2, D)

    def run_expert(expert_index):
        expert_rows = buffers[:, expert_index].reshape(N_EP * CAP, D)
        summed = jnp.zeros((N_EP * CAP, D), jnp.float32)
        for half_index in range(2):
            gate_value = jnp.dot(expert_rows, gate_halves[expert_index, half_index], preferred_element_type=jnp.float32)
            up_value = jnp.dot(expert_rows, up_halves[expert_index, half_index], preferred_element_type=jnp.float32)
            hidden = (jax.nn.silu(gate_value) * up_value).astype(jnp.bfloat16)
            partial_value = jnp.dot(hidden, down_halves[expert_index, half_index], preferred_element_type=jnp.float32).astype(jnp.bfloat16)
            summed = summed + partial_value.astype(jnp.float32)
        return summed.astype(jnp.bfloat16).reshape(N_EP, CAP, D)

    results = lax.map(run_expert, jnp.arange(EXPERTS, dtype=jnp.int32))
    per_source = jnp.swapaxes(results, 0, 1).reshape(N_EP, EXPERTS * CAP, D)

    def gather_back(table, flat_index, weights):
        picked = table[flat_index].reshape(TOK_DEV, TOP, D).astype(jnp.float32)
        return jnp.einsum('tk,tkd->td', weights.astype(jnp.float32), picked)

    mixed = jax.vmap(gather_back)(per_source, flat_all, gate_weights.reshape(N_EP, TOK_DEV, TOP))
    return mixed.reshape(TOKENS, D).astype(jnp.bfloat16)
```

```python
import jax
import jax.numpy as jnp
from jax import lax
from jax.sharding import PartitionSpec as P


def dense_gates(routes, gate_weights, expert_count):
    hit = routes[:, :, None] == jnp.arange(expert_count, dtype=jnp.int32)[None, None, :]
    return jnp.sum(jnp.where(hit, gate_weights[:, :, None], 0.0), axis=1)


def body(tokens, routes, gate_weights, w_gate, w_up, w_down):
    devices = lax.axis_size("ep")
    expert_count = devices // 2
    expert = lax.axis_index("ep") // 2
    gates = dense_gates(routes, gate_weights, expert_count)
    all_gates = lax.all_gather(gates, "ep", axis=0, tiled=True)
    mine = lax.dynamic_slice_in_dim(all_gates, expert, 1, axis=1)
    rows = lax.all_gather(tokens, "ep", axis=0, tiled=True)
    gate_value = jnp.dot(rows, w_gate[0], preferred_element_type=jnp.float32)
    up_value = jnp.dot(rows, w_up[0], preferred_element_type=jnp.float32)
    hidden = (jax.nn.silu(gate_value) * up_value * mine).astype(jnp.bfloat16)
    partial_value = jnp.dot(hidden, w_down[0], preferred_element_type=jnp.float32)
    return lax.psum_scatter(
        partial_value.astype(jnp.bfloat16), "ep", scatter_dimension=0, tiled=True
    )


def solution(mesh):
    placed = (
        P(("rep", "ep"), None),
        P(("rep", "ep"), None),
        P(("rep", "ep"), None),
        P("ep", None, None),
        P("ep", None, None),
        P("ep", None, None),
    )
    return jax.shard_map(
        body, mesh=mesh, in_specs=placed, out_specs=P(("rep", "ep"), None), check_vma=False
    )
```

```python
import functools

import jax
import jax.numpy as jnp
from jax import lax
from jax.experimental import pallas as pl
from jax.experimental.pallas import tpu as pltpu
from jax.sharding import PartitionSpec as P

F32 = jnp.float32
BF16 = jnp.bfloat16
PLANE = 4
KINDS = 15
(Z_ROWS, X_ROWS, Y_ROWS, D_LOW, D_HIGH, TWIN, _, _, _, PAIR, S_LOW, S_HIGH, S_X, S_Y, S_Z) = range(KINDS)


def pack_width(expert_count):
    return -(-3 * expert_count // 128) * 128


def packed_gates(routes, weights, expert_count, lanes):
    rows, top = routes.shape
    lane = lax.broadcasted_iota(jnp.int32, (rows, lanes), 1)
    expert = jnp.where(lane >= 2 * expert_count, lane - 2 * expert_count, jnp.where(lane >= expert_count, lane - expert_count, lane))
    dense = jnp.zeros((rows, lanes), F32)
    for k in range(top):
        dense = dense + jnp.where(routes[:, k : k + 1] == expert, weights[:, k : k + 1], 0.0)
    high = dense.astype(BF16).astype(F32)
    middle = (dense - high).astype(BF16).astype(F32)
    low = dense - high - middle
    piece = jnp.where(lane < expert_count, high, jnp.where(lane < 2 * expert_count, middle, low))
    return jnp.where(lane < 3 * expert_count, piece, 0.0).astype(BF16)


def kernel(
    devices, tokens, routes, weights, w_gate, w_up, w_down, out,
    tok, wg, wu, wd, hid, p_own, p_out, p_in, diag, low_in, high_in,
    to_x, to_y, from_x, from_y, to_z, from_z, kept, load_sem, send_sem, recv_sem,
):
    rows, width = out.shape
    planes = devices // (2 * PLANE)
    expert_count = devices // 2
    wide = tok.shape[1]
    half_w = wide // 256 * 128
    half_d = width // 256 * 128
    chunk = 2 * PLANE * rows
    near = PLANE * rows
    me = lax.axis_index("ep")
    twin = me + 1 - 2 * (me % 2)
    x_mate = me + 2 - 4 * ((me // 2) % 2)
    y_mate = me + 4 - 8 * ((me // 4) % 2)
    z, inside = me // (2 * PLANE), me % (2 * PLANE)

    def z_mate(step):
        return ((z + step) % planes) * (2 * PLANE) + inside

    loads = [
        pltpu.make_async_copy(tokens, tok.at[pl.ds(0, rows), pl.ds(0, width)], load_sem.at[0]),
        pltpu.make_async_copy(w_gate.at[0], wg, load_sem.at[1]),
        pltpu.make_async_copy(w_up.at[0], wu, load_sem.at[2]),
        pltpu.make_async_copy(w_down.at[0], wd, load_sem.at[3]),
    ]
    for load in loads:
        load.start()
    barrier = pltpu.get_barrier_semaphore()
    mates = [twin, x_mate, y_mate] + [z_mate(s) for s in range(1, planes)]
    for mate in mates:
        pl.semaphore_signal(barrier, inc=1, device_id={"ep": mate}, device_id_type=pl.DeviceIdType.MESH)
    tok[pl.ds(0, rows), pl.ds(width, wide - width)] = packed_gates(routes[...], weights[...], expert_count, wide - width)
    loads[0].wait()
    pl.semaphore_wait(barrier, len(mates))

    copies = {}

    def send(kind, s, source, target, device):
        copy = pltpu.make_async_remote_copy(
            src_ref=source, dst_ref=target,
            send_sem=send_sem.at[kind, s], recv_sem=recv_sem.at[kind, s],
            device_id={"ep": device}, device_id_type=pl.DeviceIdType.MESH,
        )
        copy.start()
        copies[kind, s] = copy

    def arrived(kind, s):
        copies[kind, s].wait_recv()

    def block(s, k, r, first=0, size=None):
        return tok.at[pl.ds(((s * 2 + k) * PLANE + r) * rows, rows), pl.ds(first, wide if size is None else size)]

    def to_twin(s, r):
        send(TWIN + r, s, block(s, 0, r), block(s, 1, r), twin)

    def gather_own(s):
        if s:
            arrived(Z_ROWS, s)
        send(X_ROWS, s, block(s, 0, 0), block(s, 0, 1), x_mate)
        send(Y_ROWS, s, block(s, 0, 0), block(s, 0, 2), y_mate)
        to_twin(s, 0)

    def gather_side(s):
        arrived(X_ROWS, s)
        send(D_LOW, s, block(s, 0, 1, 0, half_w), block(s, 0, 3, 0, half_w), y_mate)
        arrived(Y_ROWS, s)
        send(D_HIGH, s, block(s, 0, 2, half_w, wide - half_w), block(s, 0, 3, half_w, wide - half_w), x_mate)
        to_twin(s, 1)
        to_twin(s, 2)

    def gather_diag(s):
        arrived(D_LOW, s)
        arrived(D_HIGH, s)
        to_twin(s, 3)

    def compute(s):
        for r in range(PLANE):
            arrived(TWIN + r, s)
        here = pl.ds(s * chunk, chunk)
        if s == 0:
            loads[1].wait()
            loads[2].wait()
        lanes = wide - width
        lane = lax.broadcasted_iota(jnp.int32, (chunk, lanes), 1)
        expert = me // 2
        mine = (lane == expert) | (lane == expert + expert_count) | (lane == expert + 2 * expert_count)
        scale = jnp.sum(jnp.where(mine, tok[here, pl.ds(width, lanes)].astype(F32), 0.0), axis=1, keepdims=True)
        hidden_count = wg.shape[1]
        piece = min(256, hidden_count)

        def hidden_piece(j, carry):
            cols = pl.ds(pl.multiple_of(j * piece, piece), piece)
            gate = jnp.dot(tok[here, pl.ds(0, width)], wg[:, cols], preferred_element_type=F32)
            up = jnp.dot(tok[here, pl.ds(0, width)], wu[:, cols], preferred_element_type=F32)
            hid[:, cols] = (jax.nn.silu(gate) * up * scale).astype(BF16)
            return carry

        lax.fori_loop(0, hidden_count // piece, hidden_piece, 0)
        if s == 0:
            loads[3].wait()
        span = 512 if width % 512 == 0 else 128

        def down_piece(j, carry):
            cols = pl.ds(pl.multiple_of(j * span, span), span)
            part = jnp.dot(hid[...], wd[:, cols], preferred_element_type=F32)
            p_own[pl.ds(s * near, near), cols] = part[:near]
            p_out[pl.ds(s * near, near), cols] = part[near:].astype(BF16)
            return carry

        lax.fori_loop(0, width // span, down_piece, 0)
        send(PAIR, s, p_out.at[pl.ds(s * near, near), :], p_in.at[pl.ds(s * near, near), :], twin)

    def slab(s):
        return pl.ds(s * rows, rows)

    def both(s, r):
        at = pl.ds(s * near + r * rows, rows)
        return p_own[at, :] + p_in[at, :].astype(F32)

    def scatter_diag(s):
        arrived(PAIR, s)
        diag[slab(s), :] = both(s, 3).astype(BF16)
        send(S_LOW, s, diag.at[slab(s), pl.ds(0, half_d)], low_in.at[slab(s), :], y_mate)
        send(S_HIGH, s, diag.at[slab(s), pl.ds(half_d, width - half_d)], high_in.at[slab(s), :], x_mate)

    def scatter_side(s):
        for_x, for_y = both(s, 1), both(s, 2)
        arrived(S_LOW, s)
        to_x[slab(s), pl.ds(0, half_d)] = (for_x[:, :half_d] + low_in[slab(s), :].astype(F32)).astype(BF16)
        to_x[slab(s), pl.ds(half_d, width - half_d)] = for_x[:, half_d:].astype(BF16)
        send(S_X, s, to_x.at[slab(s), :], from_x.at[slab(s), :], x_mate)
        arrived(S_HIGH, s)
        to_y[slab(s), pl.ds(0, half_d)] = for_y[:, :half_d].astype(BF16)
        to_y[slab(s), pl.ds(half_d, width - half_d)] = (for_y[:, half_d:] + high_in[slab(s), :].astype(F32)).astype(BF16)
        send(S_Y, s, to_y.at[slab(s), :], from_y.at[slab(s), :], y_mate)

    def scatter_own(s):
        arrived(S_X, s)
        arrived(S_Y, s)
        total = both(s, 0) + from_x[slab(s), :].astype(F32) + from_y[slab(s), :].astype(F32)
        if s:
            to_z[slab(s), :] = total.astype(BF16)
            send(S_Z, s, to_z.at[slab(s), :], from_z.at[slab(s), :], z_mate(s))
        else:
            kept[...] = total

    for s in range(1, planes):
        send(Z_ROWS, s, block(0, 0, 0), block(s, 0, 0), z_mate(planes - s))
    stages = [(gather_own, 0), (gather_side, 1), (gather_diag, 2), (compute, 3), (scatter_diag, 4), (scatter_side, 5), (scatter_own, 6)]
    order = []
    for place, (stage, tick) in enumerate(stages):
        for s in range(planes):
            order.append((s + tick, place == 3, tick, s, stage))
    for _, _, _, s, stage in sorted(order, key=lambda item: item[:4]):
        stage(s)
    total = kept[...]
    for s in range(1, planes):
        arrived(S_Z, s)
        total = total + from_z[slab(s), :].astype(F32)
    out[...] = total.astype(BF16)
    for copy in copies.values():
        copy.wait_send()


def body(tokens, routes, gate_weights, w_gate, w_up, w_down):
    devices = lax.axis_size("ep")
    rows, width = tokens.shape
    hidden = w_gate.shape[2]
    planes = devices // (2 * PLANE)
    wide = width + pack_width(devices // 2)
    half_d = width // 256 * 128
    slab = pltpu.VMEM((planes * rows, width), BF16)
    anywhere, vmem = pl.BlockSpec(memory_space=pl.ANY), pl.BlockSpec(memory_space=pltpu.VMEM)
    return pl.pallas_call(
        functools.partial(kernel, devices),
        out_shape=jax.ShapeDtypeStruct((rows, width), BF16),
        in_specs=[anywhere, vmem, vmem, anywhere, anywhere, anywhere],
        out_specs=vmem,
        scratch_shapes=[
            pltpu.VMEM((devices * rows, wide), BF16),
            pltpu.VMEM((width, hidden), BF16),
            pltpu.VMEM((width, hidden), BF16),
            pltpu.VMEM((hidden, width), BF16),
            pltpu.VMEM((2 * PLANE * rows, hidden), BF16),
            pltpu.VMEM((devices // 2 * rows, width), F32),
            pltpu.VMEM((devices // 2 * rows, width), BF16),
            pltpu.VMEM((devices // 2 * rows, width), BF16),
            slab,
            pltpu.VMEM((planes * rows, half_d), BF16),
            pltpu.VMEM((planes * rows, width - half_d), BF16),
            slab, slab, slab, slab, slab, slab,
            pltpu.VMEM((rows, width), F32),
            pltpu.SemaphoreType.DMA((4,)),
            pltpu.SemaphoreType.DMA((KINDS, planes)),
            pltpu.SemaphoreType.DMA((KINDS, planes)),
        ],
        compiler_params=pltpu.CompilerParams(
            collective_id=0, has_side_effects=True, vmem_limit_bytes=60 * 1024 * 1024
        ),
    )(tokens, routes, gate_weights, w_gate, w_up, w_down)


def solution(mesh):
    placed = (
        P(("rep", "ep"), None),
        P(("rep", "ep"), None),
        P(("rep", "ep"), None),
        P("ep", None, None),
        P("ep", None, None),
        P("ep", None, None),
    )
    return jax.shard_map(
        body, mesh=mesh, in_specs=placed, out_specs=P(("rep", "ep"), None), check_vma=False
    )
```

```python
import functools

import jax
import jax.numpy as jnp
from jax import lax
from jax.experimental import pallas as pl
from jax.experimental.pallas import tpu as pltpu
from jax.sharding import PartitionSpec as P

F32 = jnp.float32
BF16 = jnp.bfloat16
PLANE = 4
KINDS = 15
(Z_ROWS, X_ROWS, Y_ROWS, D_LOW, D_HIGH, TWIN, _, _, _, PAIR, S_LOW, S_HIGH, S_X, S_Y, S_Z) = range(KINDS)


def pack_width(expert_count):
    return -(-3 * expert_count // 128) * 128


def packed_gates(routes, weights, expert_count, lanes):
    rows, top = routes.shape
    lane = lax.broadcasted_iota(jnp.int32, (rows, lanes), 1)
    expert = jnp.where(lane >= 2 * expert_count, lane - 2 * expert_count, jnp.where(lane >= expert_count, lane - expert_count, lane))
    dense = jnp.zeros((rows, lanes), F32)
    for k in range(top):
        dense = dense + jnp.where(routes[:, k : k + 1] == expert, weights[:, k : k + 1], 0.0)
    high = dense.astype(BF16).astype(F32)
    middle = (dense - high).astype(BF16).astype(F32)
    low = dense - high - middle
    piece = jnp.where(lane < expert_count, high, jnp.where(lane < 2 * expert_count, middle, low))
    return jnp.where(lane < 3 * expert_count, piece, 0.0).astype(BF16)


def kernel(
    devices, tokens, routes, weights, w_gate, w_up, w_down, out,
    tok, wg, wu, wd, hid, p_own, p_out, p_in, diag, low_in, high_in,
    to_x, to_y, from_x, from_y, to_z, from_z, kept, load_sem, send_sem, recv_sem,
):
    rows, width = out.shape
    planes = devices // (2 * PLANE)
    expert_count = devices // 2
    wide = tok.shape[1]
    half_w = wide // 256 * 128
    half_d = width // 256 * 128
    chunk = 2 * PLANE * rows
    near = PLANE * rows
    me = lax.axis_index("ep")
    twin = me + 1 - 2 * (me % 2)
    x_mate = me + 2 - 4 * ((me // 2) % 2)
    y_mate = me + 4 - 8 * ((me // 4) % 2)
    z, inside = me // (2 * PLANE), me % (2 * PLANE)

    def z_mate(step):
        other, bit = z, 1
        while bit < planes:
            if step & bit:
                other = other + bit * (1 - 2 * ((z // bit) % 2))
            bit *= 2
        return other * (2 * PLANE) + inside

    loads = [
        pltpu.make_async_copy(tokens, tok.at[pl.ds(0, rows), pl.ds(0, width)], load_sem.at[0]),
        pltpu.make_async_copy(w_gate.at[0], wg, load_sem.at[1]),
        pltpu.make_async_copy(w_up.at[0], wu, load_sem.at[2]),
        pltpu.make_async_copy(w_down.at[0], wd, load_sem.at[3]),
    ]
    for load in loads:
        load.start()
    barrier = pltpu.get_barrier_semaphore()
    mates = [twin, x_mate, y_mate] + [z_mate(s) for s in range(1, planes)]
    for mate in mates:
        pl.semaphore_signal(barrier, inc=1, device_id={"ep": mate}, device_id_type=pl.DeviceIdType.MESH)
    tok[pl.ds(0, rows), pl.ds(width, wide - width)] = packed_gates(routes[...].T, weights[...].T, expert_count, wide - width)
    loads[0].wait()
    pl.semaphore_wait(barrier, len(mates))

    copies = {}

    def send(kind, s, source, target, device):
        copy = pltpu.make_async_remote_copy(
            src_ref=source, dst_ref=target,
            send_sem=send_sem.at[kind, s], recv_sem=recv_sem.at[kind, s],
            device_id={"ep": device}, device_id_type=pl.DeviceIdType.MESH,
        )
        copy.start()
        copies[kind, s] = copy

    def arrived(kind, s):
        copies[kind, s].wait_recv()

    def block(s, k, r, first=0, size=None):
        return tok.at[pl.ds(((s * 2 + k) * PLANE + r) * rows, rows), pl.ds(first, wide if size is None else size)]

    def to_twin(s, r):
        send(TWIN + r, s, block(s, 0, r), block(s, 1, r), twin)

    def gather_own(s):
        if s:
            arrived(Z_ROWS, s)
        send(X_ROWS, s, block(s, 0, 0), block(s, 0, 1), x_mate)
        send(Y_ROWS, s, block(s, 0, 0), block(s, 0, 2), y_mate)
        to_twin(s, 0)

    def gather_side(s):
        arrived(X_ROWS, s)
        send(D_LOW, s, block(s, 0, 1, 0, half_w), block(s, 0, 3, 0, half_w), y_mate)
        arrived(Y_ROWS, s)
        send(D_HIGH, s, block(s, 0, 2, half_w, wide - half_w), block(s, 0, 3, half_w, wide - half_w), x_mate)
        to_twin(s, 1)
        to_twin(s, 2)

    def gather_diag(s):
        arrived(D_LOW, s)
        arrived(D_HIGH, s)
        to_twin(s, 3)

    def compute(s):
        for r in range(PLANE):
            arrived(TWIN + r, s)
        here = pl.ds(s * chunk, chunk)
        if s == 0:
            loads[1].wait()
            loads[2].wait()
        lanes = wide - width
        lane = lax.broadcasted_iota(jnp.int32, (chunk, lanes), 1)
        expert = me // 2
        mine = (lane == expert) | (lane == expert + expert_count) | (lane == expert + 2 * expert_count)
        scale = jnp.sum(jnp.where(mine, tok[here, pl.ds(width, lanes)].astype(F32), 0.0), axis=1, keepdims=True)
        hidden_count = wg.shape[1]
        piece = min(256, hidden_count)

        def hidden_piece(j, carry):
            cols = pl.ds(pl.multiple_of(j * piece, piece), piece)
            gate = jnp.dot(tok[here, pl.ds(0, width)], wg[:, cols], preferred_element_type=F32)
            up = jnp.dot(tok[here, pl.ds(0, width)], wu[:, cols], preferred_element_type=F32)
            hid[:, cols] = (jax.nn.silu(gate) * up * scale).astype(BF16)
            return carry

        lax.fori_loop(0, hidden_count // piece, hidden_piece, 0)
        if s == 0:
            loads[3].wait()
        span = 512 if width % 512 == 0 else 128

        def down_piece(j, carry):
            cols = pl.ds(pl.multiple_of(j * span, span), span)
            part = jnp.dot(hid[...], wd[:, cols], preferred_element_type=F32)
            p_own[pl.ds(s * near, near), cols] = part[:near]
            p_out[pl.ds(s * near, near), cols] = part[near:].astype(BF16)
            return carry

        lax.fori_loop(0, width // span, down_piece, 0)
        send(PAIR, s, p_out.at[pl.ds(s * near, near), :], p_in.at[pl.ds(s * near, near), :], twin)

    def slab(s):
        return pl.ds(s * rows, rows)

    def both(s, r):
        at = pl.ds(s * near + r * rows, rows)
        return p_own[at, :] + p_in[at, :].astype(F32)

    def scatter_diag(s):
        arrived(PAIR, s)
        diag[slab(s), :] = both(s, 3).astype(BF16)
        send(S_LOW, s, diag.at[slab(s), pl.ds(0, half_d)], low_in.at[slab(s), :], y_mate)
        send(S_HIGH, s, diag.at[slab(s), pl.ds(half_d, width - half_d)], high_in.at[slab(s), :], x_mate)

    def scatter_side(s):
        for_x, for_y = both(s, 1), both(s, 2)
        arrived(S_LOW, s)
        to_x[slab(s), pl.ds(0, half_d)] = (for_x[:, :half_d] + low_in[slab(s), :].astype(F32)).astype(BF16)
        to_x[slab(s), pl.ds(half_d, width - half_d)] = for_x[:, half_d:].astype(BF16)
        send(S_X, s, to_x.at[slab(s), :], from_x.at[slab(s), :], x_mate)
        arrived(S_HIGH, s)
        to_y[slab(s), pl.ds(0, half_d)] = for_y[:, :half_d].astype(BF16)
        to_y[slab(s), pl.ds(half_d, width - half_d)] = (for_y[:, half_d:] + high_in[slab(s), :].astype(F32)).astype(BF16)
        send(S_Y, s, to_y.at[slab(s), :], from_y.at[slab(s), :], y_mate)

    def scatter_own(s):
        arrived(S_X, s)
        arrived(S_Y, s)
        total = both(s, 0) + from_x[slab(s), :].astype(F32) + from_y[slab(s), :].astype(F32)
        if s:
            to_z[slab(s), :] = total.astype(BF16)
            send(S_Z, s, to_z.at[slab(s), :], from_z.at[slab(s), :], z_mate(s))
        else:
            kept[...] = total

    for s in range(1, planes):
        send(Z_ROWS, s, block(0, 0, 0), block(s, 0, 0), z_mate(s))
    order = []
    for s in range(planes):
        late = 5 + (s + planes - 1) % planes
        order += [(s, 3, s, gather_own), (s + 1, 4, s, gather_side), (s + 2, 5, s, gather_diag), (s + 3, 6, s, compute)]
        order += [(late, 2, s, scatter_diag), (late + 1, 1, s, scatter_side), (late + 2, 0, s, scatter_own)]
    for _, _, s, stage in sorted(order, key=lambda item: item[:3]):
        stage(s)
    total = kept[...]
    for s in range(1, planes):
        arrived(S_Z, s)
        total = total + from_z[slab(s), :].astype(F32)
    out[...] = total.astype(BF16)
    for copy in copies.values():
        copy.wait_send()


def body(tokens, routes, gate_weights, w_gate, w_up, w_down):
    devices = lax.axis_size("ep")
    rows, width = tokens.shape
    hidden = w_gate.shape[2]
    planes = devices // (2 * PLANE)
    wide = width + pack_width(devices // 2)
    half_d = width // 256 * 128
    slab = pltpu.VMEM((planes * rows, width), BF16)
    anywhere, vmem = pl.BlockSpec(memory_space=pl.ANY), pl.BlockSpec(memory_space=pltpu.VMEM)
    return pl.pallas_call(
        functools.partial(kernel, devices),
        out_shape=jax.ShapeDtypeStruct((rows, width), BF16),
        in_specs=[anywhere, vmem, vmem, anywhere, anywhere, anywhere],
        out_specs=vmem,
        scratch_shapes=[
            pltpu.VMEM((devices * rows, wide), BF16),
            pltpu.VMEM((width, hidden), BF16),
            pltpu.VMEM((width, hidden), BF16),
            pltpu.VMEM((hidden, width), BF16),
            pltpu.VMEM((2 * PLANE * rows, hidden), BF16),
            pltpu.VMEM((devices // 2 * rows, width), F32),
            pltpu.VMEM((devices // 2 * rows, width), BF16),
            pltpu.VMEM((devices // 2 * rows, width), BF16),
            slab,
            pltpu.VMEM((planes * rows, half_d), BF16),
            pltpu.VMEM((planes * rows, width - half_d), BF16),
            slab, slab, slab, slab, slab, slab,
            pltpu.VMEM((rows, width), F32),
            pltpu.SemaphoreType.DMA((4,)),
            pltpu.SemaphoreType.DMA((KINDS, planes)),
            pltpu.SemaphoreType.DMA((KINDS, planes)),
        ],
        compiler_params=pltpu.CompilerParams(
            collective_id=0, has_side_effects=True, vmem_limit_bytes=60 * 1024 * 1024
        ),
    )(tokens, routes.T, gate_weights.T, w_gate, w_up, w_down)


def solution(mesh):
    placed = (
        P(("rep", "ep"), None),
        P(("rep", "ep"), None),
        P(("rep", "ep"), None),
        P("ep", None, None),
        P("ep", None, None),
        P("ep", None, None),
    )
    return jax.shard_map(
        body, mesh=mesh, in_specs=placed, out_specs=P(("rep", "ep"), None), check_vma=False
    )
```
